32 devices in a mesh: seq: 16 (over z, x, core), grp: 2 (over y).
Axes of the slice: x: 2, y: 2, z: 4, core: 2. Of those that a mesh axis runs over, the one named last changes fastest.
Arguments:
- out_grad: bfloat16 [2, 3456, 1024], P('grp', 'seq'), may hold values from -6 to 6
- combine_logits: float32 [2, 3456, 64], P('grp', 'seq'), may hold values from -20 to 330
- expert_out: bfloat16 [2, 64, 1024], P('grp', 'seq'), may hold values from -6 to 6
- slot_in: bfloat16 [2, 64, 1024], P('grp', 'seq'), may hold values from -6 to 6
- router: bfloat16 [64, 1024], P('seq'), may hold values from -0.1875 to 0.1875
- w_gate: bfloat16 [64, 2048, 1024], P('seq', 'grp'), may hold values from -0.1875 to 0.1875
- w_up: bfloat16 [64, 2048, 1024], P('seq', 'grp'), may hold values from -0.1875 to 0.1875
- w_down: bfloat16 [64, 2048, 1024], P('seq', 'grp'), may hold values from -0.125 to 0.125
Outputs:
- token_grad: bfloat16 [2, 3456, 1024], P('grp', 'seq')
- slot_grad: float32 [2, 64, 1024], P('grp', 'seq')
- grad_gate: bfloat16 [64, 2048, 1024], P('seq', 'grp')
- grad_up: bfloat16 [64, 2048, 1024], P('seq', 'grp')
- grad_down: bfloat16 [64, 2048, 1024], P('seq', 'grp')
The draws below stay inside these ranges and needn't reach their ends.
All inputs are finite; a program needn't handle non-finite values.
Results may differ from the reference program's by a relative error of at most 0.028.
Values may be sent and summed in bfloat16 or wider, within the bound.
No kernel may reach another device: no remote copies, remote signals or barrier semaphores. Data moves between devices by JAX's collectives and lax.ppermute only.
A program may use at most 128 MiB of HBM per device.

```python
import jax
import jax.numpy as jnp
from jax import lax

D = 1024
FF = 2048
EXPERTS = 64
TOKENS = 3456
SEQS = 2


def draw_combine_logits(key, part):
    keys = jax.random.split(key, 1)
    shape = (SEQS, TOKENS, EXPERTS)
    return jnp.clip(3.0 * jax.random.normal(keys[0], shape, jnp.float32), -18.0, 18.0)


def shard_levels(stream_key, shape, cuts, least, top_value):
    loudness = 1.0
    for dim, blocks in cuts:
        draws = jax.random.uniform(jax.random.fold_in(jax.random.fold_in(stream_key, 6), dim), (blocks,), jnp.float32, least / len(cuts), top_value / len(cuts))
        loudness = loudness * jnp.repeat(jnp.exp(draws), shape[dim] // blocks).reshape((-1,) + (1,) * (len(shape) - 1 - dim))
    return loudness


def centred(key, shape, spread, limit, cuts=(), kind=jnp.bfloat16):
    result = spread * jax.random.normal(key, shape, jnp.float32)
    if cuts:
        result = result * shard_levels(key, shape, cuts, -0.22, 0.18)
    return jnp.clip(result, -limit, limit).astype(kind)


def setup_inputs(seed: int = 0) -> dict:
    seeds = jax.random.split(jax.random.key(seed), 9)
    out_grad = centred(seeds[0], (SEQS, TOKENS, D), 1.0, 6.0, ((0, 2), (1, 16)))
    combine_logits = draw_combine_logits(jax.random.fold_in(seeds[8], 71), 0)
    expert_out = centred(seeds[2], (SEQS, EXPERTS, D), 1.0, 6.0, ((0, 2), (1, 16)))
    slot_in = centred(seeds[3], (SEQS, EXPERTS, D), 1.0, 6.0, ((0, 2), (1, 16)))
    router = centred(seeds[4], (EXPERTS, D), D ** -0.5, 0.1875, ((0, 16),))
    w_gate = centred(seeds[5], (EXPERTS, FF, D), D ** -0.5, 0.1875, ((0, 16), (1, 2)))
    w_up = centred(seeds[6], (EXPERTS, FF, D), D ** -0.5, 0.1875, ((0, 16), (1, 2)))
    w_down = centred(seeds[7], (EXPERTS, FF, D), FF ** -0.5, 0.125, ((0, 16), (1, 2)))
    return dict(out_grad=out_grad, combine_logits=combine_logits, expert_out=expert_out, slot_in=slot_in, router=router, w_gate=w_gate, w_up=w_up, w_down=w_down)


def sequence_part(items, router):
    grads, logits, outputs = items
    probs = jax.nn.softmax(logits, axis=-1)
    probs_bf = probs.astype(jnp.bfloat16)
    slot_out = lax.dot_general(probs_bf, grads, (((0,), (0,)), ((), ())), preferred_element_type=jnp.float32)
    weight_grad = lax.dot_general(grads, outputs, (((1,), (1,)), ((), ())), preferred_element_type=jnp.float32)
    centre = jnp.sum(weight_grad * probs, axis=-1, keepdims=True)
    logit_grad = (probs * (weight_grad - centre)).astype(jnp.bfloat16)
    token_grad = jnp.dot(logit_grad, router, preferred_element_type=jnp.float32).astype(jnp.bfloat16)
    return token_grad, slot_out.astype(jnp.bfloat16)


def expert_part(items):
    inputs, out_grads, w_gate, w_up, w_down = items
    dims = (((1,), (1,)), ((), ()))
    gate = lax.dot_general(inputs, w_gate, dims, preferred_element_type=jnp.float32)
    upper = lax.dot_general(inputs, w_up, dims, preferred_element_type=jnp.float32)
    sig = jax.nn.sigmoid(gate)
    hidden = (gate * sig * upper).astype(jnp.bfloat16)
    hidden_grad = lax.dot_general(out_grads, w_down, dims, preferred_element_type=jnp.float32)
    up_grad = (hidden_grad * gate * sig).astype(jnp.bfloat16)
    gate_grad = (hidden_grad * upper * sig * (1.0 + gate * (1.0 - sig))).astype(jnp.bfloat16)
    slot_grad = jnp.dot(gate_grad, w_gate, preferred_element_type=jnp.float32) + jnp.dot(up_grad, w_up, preferred_element_type=jnp.float32)
    outer = (((0,), (0,)), ((), ()))
    grad_gate = lax.dot_general(gate_grad, inputs, outer, preferred_element_type=jnp.float32).astype(jnp.bfloat16)
    grad_up = lax.dot_general(up_grad, inputs, outer, preferred_element_type=jnp.float32).astype(jnp.bfloat16)
    grad_down = lax.dot_general(hidden, out_grads, outer, preferred_element_type=jnp.float32).astype(jnp.bfloat16)
    return slot_grad, grad_gate, grad_up, grad_down


def reference(out_grad, combine_logits, expert_out, slot_in, router, w_gate, w_up, w_down):
    token_grad, slot_out_bf = lax.map(lambda items: sequence_part(items, router), (out_grad, combine_logits, expert_out))
    per_expert = (jnp.transpose(slot_in, (1, 0, 2)), jnp.transpose(slot_out_bf, (1, 0, 2)), w_gate, w_up, w_down)
    slot_grad, grad_gate, grad_up, grad_down = lax.map(expert_part, per_expert)
    return token_grad, jnp.transpose(slot_grad, (1, 0, 2)), grad_gate, grad_up, grad_down
```

```python
import jax
import jax.numpy as jnp
from jax import lax
from jax.sharding import PartitionSpec as P

F32 = jnp.float32
BF16 = jnp.bfloat16


def shifted(x, size, k):
    return lax.ppermute(x, "grp", [((i + k) % size, i) for i in range(size)])


def slot_backward(inputs, out_grads, w_gate, w_up, w_down):
    gate = jnp.einsum("ged,efd->gef", inputs, w_gate, preferred_element_type=F32)
    upper = jnp.einsum("ged,efd->gef", inputs, w_up, preferred_element_type=F32)
    sig = jax.nn.sigmoid(gate)
    hidden = (gate * sig * upper).astype(BF16)
    hidden_grad = jnp.einsum("ged,efd->gef", out_grads, w_down, preferred_element_type=F32)
    up_grad = (hidden_grad * gate * sig).astype(BF16)
    gate_grad = (hidden_grad * upper * sig * (1.0 + gate * (1.0 - sig))).astype(BF16)
    partial_grad = jnp.einsum("gef,efd->ged", gate_grad, w_gate, preferred_element_type=F32)
    partial_grad = partial_grad + jnp.einsum("gef,efd->ged", up_grad, w_up, preferred_element_type=F32)
    grad_gate = jnp.einsum("gef,ged->efd", gate_grad, inputs, preferred_element_type=F32).astype(BF16)
    grad_up = jnp.einsum("gef,ged->efd", up_grad, inputs, preferred_element_type=F32).astype(BF16)
    grad_down = jnp.einsum("gef,ged->efd", hidden, out_grads, preferred_element_type=F32).astype(BF16)
    return partial_grad, grad_gate, grad_up, grad_down


def per_device(n_seq, n_grp, out_grad, combine_logits, expert_out, slot_in, router, w_gate, w_up, w_down):
    grads = out_grad[0]
    own, width = router.shape
    inputs = jnp.stack([slot_in[0]] + [shifted(slot_in[0], n_grp, k) for k in range(1, n_grp)])
    probs = jax.nn.softmax(combine_logits[0], axis=-1)
    partial = lax.dot_general(probs.astype(BF16), grads, (((0,), (0,)), ((), ())), preferred_element_type=F32)
    parts = lax.all_to_all(
        partial.astype(BF16).reshape(n_seq, own, width), "seq", split_axis=0, concat_axis=0, tiled=True
    )
    mine = jnp.concatenate([expert_out[0], router], axis=0)
    every = lax.all_to_all(
        jnp.broadcast_to(mine[None], (n_seq, 2 * own, width)), "seq", split_axis=0, concat_axis=0, tiled=True
    )
    outputs = every[:, :own].reshape(n_seq * own, width)
    routers = every[:, own:].reshape(n_seq * own, width)
    weight_grad = lax.dot_general(grads, outputs, (((1,), (1,)), ((), ())), preferred_element_type=F32)
    centre = jnp.sum(weight_grad * probs, axis=-1, keepdims=True)
    logit_grad = (probs * (weight_grad - centre)).astype(BF16)
    token_grad = jnp.dot(logit_grad, routers, preferred_element_type=F32).astype(BF16)[None]
    slot_out = jnp.sum(parts.astype(F32), axis=0).astype(BF16)
    all_out = jnp.stack([slot_out] + [shifted(slot_out, n_grp, k) for k in range(1, n_grp)])
    partial_grad, grad_gate, grad_up, grad_down = slot_backward(inputs, all_out, w_gate, w_up, w_down)
    slot_grad = partial_grad[0]
    for k in range(1, n_grp):
        slot_grad = slot_grad + shifted(partial_grad[k].astype(BF16), n_grp, n_grp - k).astype(F32)
    return token_grad, slot_grad[None], grad_gate, grad_up, grad_down


def solution(mesh):
    def body(*args):
        return per_device(mesh.shape["seq"], mesh.shape["grp"], *args)

    tokens, weights = P("grp", "seq", None), P("seq", "grp", None)
    return jax.shard_map(
        body,
        mesh=mesh,
        in_specs=(tokens, tokens, tokens, tokens, P("seq", None), weights, weights, weights),
        out_specs=(tokens, tokens, weights, weights, weights),
        check_vma=False,
    )
```

```python
import functools

import jax
import jax.numpy as jnp
from jax import lax
from jax.experimental import pallas as pl
from jax.experimental.pallas import tpu as pltpu
from jax.sharding import PartitionSpec as P

F32 = jnp.float32
BF16 = jnp.bfloat16
VMEM = pl.BlockSpec(memory_space=pltpu.VMEM)
HBM = pl.BlockSpec(memory_space=pltpu.HBM)
SEMS = pltpu.SemaphoreType.DMA


def shape(dims, kind):
    return jax.ShapeDtypeStruct(dims, kind)


def in_hbm(x):
    return pltpu.with_memory_space_constraint(x, pltpu.HBM)


def dot(a, b, contract):
    return lax.dot_general(a, b, (contract, ((), ())), preferred_element_type=F32)


def start(src, dst, sem):
    copy = pltpu.make_async_copy(src, dst, sem)
    copy.start()
    return copy


def call(body, name, outs, out_specs, args, in_specs, scratch=(), us=1.0, vmem=8 << 20):
    return pl.pallas_call(
        body,
        name=name,
        out_shape=outs,
        in_specs=in_specs,
        out_specs=out_specs,
        scratch_shapes=scratch,
        compiler_params=pltpu.CompilerParams(vmem_limit_bytes=vmem),
        cost_estimate=pl.CostEstimate(flops=int(us * 8e8), bytes_accessed=int(us * 3e6), transcendentals=0),
    )(*args)


def soft_kernel(logits_hbm, grads_hbm, outputs_hbm, router_hbm, x_hbm, probs_ref, all_hbm, x_ref,
                logits_ref, grads_ref, both_ref, parts_ref, sems, both_sems, parts_sems):
    loads = [
        start(outputs_hbm, both_ref.at[0], sems.at[2]),
        start(router_hbm, both_ref.at[1], sems.at[3]),
        start(logits_hbm, logits_ref, sems.at[0]),
        start(grads_hbm, grads_ref, sems.at[1]),
        start(x_hbm, x_ref, sems.at[4]),
    ]
    n, own, _ = parts_ref.shape
    loads[0].wait()
    loads[1].wait()
    copies = [start(both_ref, all_hbm.at[pl.ds(3 * j + 1, 2)], both_sems.at[j]) for j in range(n)]
    loads[2].wait()
    logits = logits_ref[...]
    weights = jnp.exp(logits - jnp.max(logits, axis=0, keepdims=True))
    probs = weights / jnp.sum(weights, axis=0, keepdims=True)
    probs_ref[...] = probs
    loads[3].wait()
    partial = dot(probs.astype(BF16), grads_ref[...], ((1,), (0,))).astype(BF16)
    for j in range(n):
        parts_ref[j] = partial[j * own : (j + 1) * own]
    copies += [start(parts_ref.at[j], all_hbm.at[3 * j], parts_sems.at[j]) for j in range(n)]
    for copy in copies + loads[4:]:
        copy.wait()


def forward_kernel(n_grp, *refs):
    x_refs = refs[:n_grp]
    w_gate_hbm, w_up_hbm, gate_ref, up_ref, w_gate_ref, w_up_ref, sems = refs[n_grp:]
    experts = gate_ref.shape[0]
    pairs = ((w_gate_hbm, w_gate_ref), (w_up_hbm, w_up_ref))
    copies = [[start(s.at[e], d.at[e], sems.at[i, e]) for i, (s, d) in enumerate(pairs)] for e in range(experts)]
    for e in range(experts):
        x = jnp.concatenate([r[e : e + 1] for r in x_refs], axis=0)
        copies[e][0].wait()
        gate_ref[e] = dot(x, w_gate_ref[e], ((1,), (1,)))
        copies[e][1].wait()
        up_ref[e] = dot(x, w_up_ref[e], ((1,), (1,)))


def load_kernel(so_ref, *refs):
    count = (len(refs) - 2) // 2
    pairs = tuple(zip(refs[:count], refs[count : 2 * count]))
    same_ref, sems = refs[2 * count :]
    copies = [start(s.at[e], d.at[e], sems.at[i, e]) for i, (s, d) in enumerate(pairs) for e in range(d.shape[0])]
    same_ref[...] = so_ref[...]
    for copy in copies:
        copy.wait()


def outer(left, right):
    n, rows = left.shape
    pad = -n % 8
    tall = left if pad == 0 else jnp.concatenate([left, jnp.zeros((pad, rows), F32)], axis=0)
    tall = tall.T
    total = tall[:, 0:1] * right[0:1]
    for s in range(1, n):
        total = total + tall[:, s : s + 1] * right[s : s + 1]
    return total.astype(BF16)


def put(value, buf_ref, out_hbm, sems, e, b):
    block = value.shape[0]
    span = pl.ds(b * block, block)
    buf_ref[e, span] = value
    start(buf_ref.at[e, span], out_hbm.at[e, span], sems.at[e, b])


def drain(out_hbm, buf_ref, sems):
    experts, blocks = sems.shape
    block = buf_ref.shape[1] // blocks

    @pl.loop(0, experts)
    def _(e):
        for b in range(blocks):
            span = pl.ds(b * block, block)
            pltpu.make_async_copy(buf_ref.at[e, span], out_hbm.at[e, span], sems.at[e, b]).wait()


def stack_rows(refs, into_ref):
    for e in range(into_ref.shape[0]):
        into_ref[e] = jnp.concatenate([r[e : e + 1] for r in refs], axis=0)


def middle_kernel(n_grp, block, *refs):
    so_refs, x_refs = refs[:n_grp], refs[n_grp : 2 * n_grp]
    gate_ref, up_ref, w_gate_hbm, w_up_hbm, w_down_ref = refs[2 * n_grp : 2 * n_grp + 5]
    partial_refs = refs[2 * n_grp + 5 : 3 * n_grp + 5]
    (up_grad_ref, grad_down_hbm, grad_gate_hbm, so_ref, x_ref, sum_ref, w_gate_ref, w_up_ref, down_buf, gate_buf,
     w_gate_sems, w_up_sems, down_sems, gate_sems) = refs[3 * n_grp + 5 :]
    experts, _, rows = gate_ref.shape
    blocks = rows // block

    def w_gate_copy(e):
        return pltpu.make_async_copy(w_gate_hbm.at[e], w_gate_ref.at[e], w_gate_sems.at[e])

    def w_up_copy(e):
        return pltpu.make_async_copy(w_up_hbm.at[e], w_up_ref.at[e], w_up_sems.at[e])

    for e in range(experts):
        w_gate_copy(e).start()
        w_up_copy(e).start()
    stack_rows(so_refs, so_ref)
    stack_rows(x_refs, x_ref)
    sum_ref[...] = jnp.zeros_like(sum_ref)

    def at(i):
        e, b = lax.div(i, blocks), lax.rem(i, blocks)
        return e, b, pl.ds(pl.multiple_of(b * block, block), block)

    def hidden_grad_at(i):
        e, b, span = at(i)
        return dot(so_ref[e], w_down_ref[e, span], ((1,), (1,)))

    def step(i, hidden_grad):
        e, b, span = at(i)

        @pl.when(b == 0)
        def _():
            w_gate_copy(e).wait()
            w_up_copy(e).wait()

        later = hidden_grad_at(jnp.minimum(i + 1, experts * blocks - 1))
        gate, up = gate_ref[e, :, span], up_ref[e, :, span]
        sig = 1.0 / (1.0 + jnp.exp(-gate))
        hidden = (gate * sig * up).astype(BF16)
        up_grad = (hidden_grad * gate * sig).astype(BF16)
        gate_grad = (hidden_grad * up * sig * (1.0 + gate * (1.0 - sig))).astype(BF16)
        up_grad_ref[e, :, span] = up_grad
        sum_ref[e] += dot(gate_grad, w_gate_ref[e, span], ((1,), (0,))) + dot(
            up_grad, w_up_ref[e, span], ((1,), (0,))
        )
        down_buf[e, span] = outer(hidden.astype(F32), so_ref[e].astype(F32))
        gate_buf[e, span] = outer(gate_grad.astype(F32), x_ref[e].astype(F32))
        start(down_buf.at[e, span], grad_down_hbm.at[e, span], down_sems.at[e, b])
        start(gate_buf.at[e, span], grad_gate_hbm.at[e, span], gate_sems.at[e, b])
        return later

    lax.fori_loop(0, experts * blocks, step, hidden_grad_at(0))
    for e in range(experts):
        for s, ref in enumerate(partial_refs):
            ref[e : e + 1] = sum_ref[e, s : s + 1].astype(ref.dtype)
    drain(grad_down_hbm, down_buf, down_sems)
    drain(grad_gate_hbm, gate_buf, gate_sems)


def last_kernel(n_grp, block, *refs):
    x_refs = refs[:n_grp]
    (up_grad_ref, probs_ref, grads_hbm, every_ref, partial_ref, grad_up_hbm, token_hbm, same_ref,
     x_ref, up_buf, grads_ref, token_ref, up_sems, sems) = refs[n_grp:]
    experts, _, rows = up_grad_ref.shape
    loaded = start(grads_hbm, grads_ref, sems.at[0])
    same_ref[...] = partial_ref[...]
    stack_rows(x_refs, x_ref)

    @pl.loop(0, experts)
    def _(e):
        x_wide = x_ref[e].astype(F32)
        for b in range(rows // block):
            up_grad = up_grad_ref[e, :, b * block : (b + 1) * block].astype(F32)
            put(outer(up_grad, x_wide), up_buf, grad_up_hbm, up_sems, e, b)

    probs = probs_ref[...]
    n = every_ref.shape[0] // 3
    outputs = jnp.concatenate([every_ref[3 * j + 1] for j in range(n)], axis=0)
    routers = jnp.concatenate([every_ref[3 * j + 2] for j in range(n)], axis=0)
    loaded.wait()
    weight_grad = dot(outputs, grads_ref[...], ((1,), (1,)))
    centre = jnp.sum(weight_grad * probs, axis=0, keepdims=True)
    logit_grad = (probs * (weight_grad - centre)).astype(BF16)
    token_ref[...] = dot(logit_grad, routers, ((0,), (0,))).astype(BF16)
    tokens = start(token_ref, token_hbm, sems.at[1])
    drain(grad_up_hbm, up_buf, up_sems)
    tokens.wait()


def shifted(x, size, k):
    return lax.ppermute(x, "grp", [((i + k) % size, i) for i in range(size)])


def per_device(n_seq, n_grp, out_grad, combine_logits, expert_out, slot_in, router, w_gate, w_up, w_down):
    grads = out_grad[0]
    own, width = router.shape
    rows = w_gate.shape[1]
    tokens = grads.shape[0]
    slots = n_seq * own
    block = min(256, rows)
    vec = (own, n_grp, rows)
    held = pltpu.VMEM((own, rows, width), BF16)
    big = shape((own, rows, width), BF16)
    buf = pltpu.VMEM((own, rows, width), BF16)
    few = pltpu.VMEM((own, n_grp, width), BF16)
    held_tokens = pltpu.VMEM((tokens, width), BF16)
    sems = SEMS((own, rows // block))
    probs, partial, x_own = call(
        soft_kernel, "soft",
        (shape((slots, tokens), F32), shape((3 * n_seq, own, width), BF16), shape((own, width), BF16)),
        (VMEM, HBM, VMEM),
        tuple(map(in_hbm, (combine_logits[0].T, grads, expert_out[0], router, slot_in[0]))), (HBM,) * 5,
        scratch=(pltpu.VMEM((slots, tokens), F32), held_tokens, pltpu.VMEM((2, own, width), BF16),
                 pltpu.VMEM((n_seq, own, width), BF16), SEMS((5,)), SEMS((n_seq,)), SEMS((n_seq,))),
    )
    every = lax.all_to_all(partial, "seq", split_axis=0, concat_axis=0, tiled=True)
    inputs = [x_own] + [shifted(x_own, n_grp, k) for k in range(1, n_grp)]
    gate, up = call(
        functools.partial(forward_kernel, n_grp), "forward", (shape(vec, F32), shape(vec, F32)), (VMEM, VMEM),
        (*inputs, in_hbm(w_gate), in_hbm(w_up)), (VMEM,) * n_grp + (HBM, HBM), scratch=(buf, buf, SEMS((2, own))),
        us=6, vmem=24 << 20,
    )
    slot_out = jnp.sum(every.reshape(n_seq, 3, own, width)[:, 0].astype(F32), axis=0).astype(BF16)
    others = [shifted(slot_out, n_grp, k) for k in range(1, n_grp)]
    w_down_v, same = call(
        load_kernel, "load", (held, shape((own, width), BF16)), (VMEM, VMEM),
        (slot_out, in_hbm(w_down)), (VMEM, HBM), scratch=(SEMS((1, own)),), us=3,
    )
    all_out = [same] + others
    *partials, up_grad, grad_down, grad_gate = call(
        functools.partial(middle_kernel, n_grp, block), "middle",
        (shape((own, width), F32),) + (shape((own, width), BF16),) * (n_grp - 1) + (shape(vec, BF16), big, big),
        (VMEM,) * (n_grp + 1) + (HBM, HBM),
        (*all_out, *inputs, gate, up, in_hbm(w_gate), in_hbm(w_up), w_down_v),
        (VMEM,) * (2 * n_grp + 2) + (HBM, HBM, VMEM),
        scratch=(few, few, pltpu.VMEM((own, n_grp, width), F32), buf, buf, buf, buf,
                 SEMS((own,)), SEMS((own,)), sems, sems),
        us=8, vmem=40 << 20,
    )
    with jax.named_scope("back"):
        back = [shifted(partials[k], n_grp, n_grp - k) for k in range(1, n_grp)]
    with jax.named_scope("ending"):
        grad_up, token_grad, slot_grad = call(
            functools.partial(last_kernel, n_grp, block), "last",
            (big, shape((tokens, width), BF16), shape((own, width), F32)), (HBM, HBM, VMEM),
            (*inputs, up_grad, probs, in_hbm(grads), every, partials[0]),
            (VMEM,) * (n_grp + 2) + (HBM, VMEM, VMEM),
            scratch=(few, buf, held_tokens, held_tokens, sems, SEMS((2,))), us=5, vmem=24 << 20,
        )
    for part in back:
        slot_grad = slot_grad + part.astype(F32)
    return token_grad[None], slot_grad[None], grad_gate, grad_up, grad_down


def solution(mesh):
    def body(*args):
        return per_device(mesh.shape["seq"], mesh.shape["grp"], *args)

    tokens, weights = P("grp", "seq", None), P("seq", "grp", None)
    return jax.shard_map(
        body,
        mesh=mesh,
        in_specs=(tokens, tokens, tokens, tokens, P("seq", None), weights, weights, weights),
        out_specs=(tokens, tokens, weights, weights, weights),
        check_vma=False,
    )
```

```python
import functools

import jax
import jax.numpy as jnp
from jax import lax
from jax.experimental import pallas as pl
from jax.experimental.pallas import tpu as pltpu
from jax.sharding import PartitionSpec as P

F32 = jnp.float32
BF16 = jnp.bfloat16
VMEM = pl.BlockSpec(memory_space=pltpu.VMEM)
HBM = pl.BlockSpec(memory_space=pltpu.HBM)
SEMS = pltpu.SemaphoreType.DMA


def shape(dims, kind):
    return jax.ShapeDtypeStruct(dims, kind)


def in_hbm(x):
    return pltpu.with_memory_space_constraint(x, pltpu.HBM)


def dot(a, b, contract):
    return lax.dot_general(a, b, (contract, ((), ())), preferred_element_type=F32)


def start(src, dst, sem):
    copy = pltpu.make_async_copy(src, dst, sem)
    copy.start()
    return copy


def call(body, name, outs, out_specs, args, in_specs, scratch=(), us=1.0, vmem=8 << 20):
    return pl.pallas_call(
        body,
        name=name,
        out_shape=outs,
        in_specs=in_specs,
        out_specs=out_specs,
        scratch_shapes=scratch,
        compiler_params=pltpu.CompilerParams(vmem_limit_bytes=vmem),
        cost_estimate=pl.CostEstimate(flops=int(us * 8e8), bytes_accessed=int(us * 3e6), transcendentals=0),
    )(*args)


def soft_kernel(logits_hbm, grads_hbm, outputs_hbm, router_hbm, x_hbm, probs_ref, all_hbm, x_ref,
                logits_ref, grads_ref, both_ref, parts_ref, sems, both_sems, parts_sems):
    loads = [
        start(outputs_hbm, both_ref.at[0], sems.at[2]),
        start(router_hbm, both_ref.at[1], sems.at[3]),
        start(logits_hbm, logits_ref, sems.at[0]),
        start(grads_hbm, grads_ref, sems.at[1]),
        start(x_hbm, x_ref, sems.at[4]),
    ]
    n, own, _ = parts_ref.shape
    loads[0].wait()
    loads[1].wait()
    copies = [start(both_ref, all_hbm.at[pl.ds(3 * j + 1, 2)], both_sems.at[j]) for j in range(n)]
    loads[2].wait()
    logits = logits_ref[...]
    weights = jnp.exp(logits - jnp.max(logits, axis=0, keepdims=True))
    probs = weights / jnp.sum(weights, axis=0, keepdims=True)
    probs_ref[...] = probs
    loads[3].wait()
    partial = dot(probs.astype(BF16), grads_ref[...], ((1,), (0,))).astype(BF16)
    for j in range(n):
        parts_ref[j] = partial[j * own : (j + 1) * own]
    copies += [start(parts_ref.at[j], all_hbm.at[3 * j], parts_sems.at[j]) for j in range(n)]
    for copy in copies + loads[4:]:
        copy.wait()


def forward_kernel(n_grp, *refs):
    x_refs = refs[:n_grp]
    w_gate_hbm, w_up_hbm, gate_ref, up_ref, w_gate_ref, w_up_ref, sems = refs[n_grp:]
    experts = gate_ref.shape[0]
    pairs = ((w_gate_hbm, w_gate_ref), (w_up_hbm, w_up_ref))
    copies = [[start(s.at[e], d.at[e], sems.at[i, e]) for i, (s, d) in enumerate(pairs)] for e in range(experts)]
    for e in range(experts):
        x = jnp.concatenate([r[e : e + 1] for r in x_refs], axis=0)
        copies[e][0].wait()
        gate_ref[e] = dot(x, w_gate_ref[e], ((1,), (1,)))
        copies[e][1].wait()
        up_ref[e] = dot(x, w_up_ref[e], ((1,), (1,)))


def sum_kernel(every_ref, after_ref, out_ref):
    del after_ref
    total = every_ref[0].astype(F32)
    for j in range(3, every_ref.shape[0], 3):
        total = total + every_ref[j].astype(F32)
    out_ref[...] = total.astype(BF16)


def pause_kernel(x_ref, same_ref):
    same_ref[...] = x_ref[...]


def outer_into(left, right, buf_ref, e, block=256):
    n, rows = left.shape
    pad = -n % 8
    tall = left if pad == 0 else jnp.concatenate([left, jnp.zeros((pad, rows), F32)], axis=0)
    tall, right = tall.T.astype(BF16), right.astype(BF16)
    block = min(block, rows)
    for b in range(0, rows, block):
        part = tall[b : b + block]
        total = part[:, 0:1] * right[0:1]
        for s in range(1, n):
            total = total + part[:, s : s + 1] * right[s : s + 1]
        buf_ref[e, pl.ds(b, block)] = total


def send(buf_ref, out_hbm, sems, e):
    blocks = sems.shape[1]
    block = buf_ref.shape[1] // blocks
    for b in range(blocks):
        span = pl.ds(b * block, block)
        start(buf_ref.at[e, span], out_hbm.at[e, span], sems.at[e, b])


def drain(out_hbm, buf_ref, sems):
    experts, blocks = sems.shape
    block = buf_ref.shape[1] // blocks

    @pl.loop(0, experts)
    def _(e):
        for b in range(blocks):
            span = pl.ds(b * block, block)
            pltpu.make_async_copy(buf_ref.at[e, span], out_hbm.at[e, span], sems.at[e, b]).wait()


def stack_rows(refs, into_ref):
    for e in range(into_ref.shape[0]):
        into_ref[e] = jnp.concatenate([r[e : e + 1] for r in refs], axis=0)


def middle_kernel(n_grp, *refs):
    so_refs, x_refs = refs[:n_grp], refs[n_grp : 2 * n_grp]
    gate_ref, up_ref, w_gate_hbm, w_up_ref, w_down_ref = refs[2 * n_grp : 2 * n_grp + 5]
    partial_refs = refs[2 * n_grp + 5 : 3 * n_grp + 5]
    (up_grad_ref, grad_down_hbm, grad_gate_hbm, so_ref, x_ref, sum_ref, w_gate_ref, down_buf, gate_buf,
     w_gate_sems, down_sems, gate_sems) = refs[3 * n_grp + 5 :]
    experts = gate_ref.shape[0]

    def w_gate_copy(e):
        return pltpu.make_async_copy(w_gate_hbm.at[e], w_gate_ref.at[e], w_gate_sems.at[e])

    for e in range(experts):
        w_gate_copy(e).start()
    stack_rows(so_refs, so_ref)
    stack_rows(x_refs, x_ref)

    def hidden_grad_of(e):
        return dot(so_ref[e], w_down_ref[e], ((1,), (1,)))

    def step(e, hidden_grad):
        w_gate_copy(e).wait()
        gate, up = gate_ref[e], up_ref[e]
        sig = 1.0 / (1.0 + jnp.exp(-gate))
        hidden = (gate * sig * up).astype(BF16)
        up_grad = (hidden_grad * gate * sig).astype(BF16)
        gate_grad = (hidden_grad * up * sig * (1.0 + gate * (1.0 - sig))).astype(BF16)
        up_grad_ref[e] = up_grad
        later = hidden_grad_of(min(e + 1, experts - 1))
        sum_ref[e] = dot(gate_grad, w_gate_ref[e], ((1,), (0,))) + dot(up_grad, w_up_ref[e], ((1,), (0,)))
        outer_into(hidden.astype(F32), so_ref[e].astype(F32), down_buf, e)
        outer_into(gate_grad.astype(F32), x_ref[e].astype(F32), gate_buf, e)
        send(down_buf, grad_down_hbm, down_sems, e)
        send(gate_buf, grad_gate_hbm, gate_sems, e)
        return later

    later = hidden_grad_of(0)
    for e in range(experts):
        later = step(e, later)
    for e in range(experts):
        for s, ref in enumerate(partial_refs):
            ref[e : e + 1] = sum_ref[e, s : s + 1].astype(ref.dtype)
    drain(grad_down_hbm, down_buf, down_sems)
    drain(grad_gate_hbm, gate_buf, gate_sems)


def last_kernel(n_grp, *refs):
    x_refs = refs[:n_grp]
    (up_grad_ref, probs_ref, grads_hbm, every_ref, partial_ref, grad_up_hbm, token_hbm, same_ref,
     x_ref, up_buf, grads_ref, token_ref, up_sems, sems) = refs[n_grp:]
    experts = up_grad_ref.shape[0]
    loaded = start(grads_hbm, grads_ref, sems.at[0])
    same_ref[...] = partial_ref[...]
    stack_rows(x_refs, x_ref)

    @pl.loop(0, experts)
    def _(e):
        outer_into(up_grad_ref[e].astype(F32), x_ref[e].astype(F32), up_buf, e)
        send(up_buf, grad_up_hbm, up_sems, e)

    probs = probs_ref[...]
    n = every_ref.shape[0] // 3
    outputs = jnp.concatenate([every_ref[3 * j + 1] for j in range(n)], axis=0)
    routers = jnp.concatenate([every_ref[3 * j + 2] for j in range(n)], axis=0)
    loaded.wait()
    weight_grad = dot(outputs, grads_ref[...], ((1,), (1,)))
    centre = jnp.sum(weight_grad * probs, axis=0, keepdims=True)
    logit_grad = (probs * (weight_grad - centre)).astype(BF16)
    token_ref[...] = dot(logit_grad, routers, ((0,), (0,))).astype(BF16)
    tokens = start(token_ref, token_hbm, sems.at[1])
    drain(grad_up_hbm, up_buf, up_sems)
    tokens.wait()


def shifted(x, size, k):
    return lax.ppermute(x, "grp", [((i + k) % size, i) for i in range(size)])


def per_device(n_seq, n_grp, out_grad, combine_logits, expert_out, slot_in, router, w_gate, w_up, w_down):
    grads = out_grad[0]
    own, width = router.shape
    rows = w_gate.shape[1]
    tokens = grads.shape[0]
    slots = n_seq * own
    block = min(256, rows)
    vec = (own, n_grp, rows)
    held = pltpu.VMEM((own, rows, width), BF16)
    big = shape((own, rows, width), BF16)
    buf = pltpu.VMEM((own, rows, width), BF16)
    few = pltpu.VMEM((own, n_grp, width), BF16)
    held_tokens = pltpu.VMEM((tokens, width), BF16)
    sems = SEMS((own, rows // block))
    probs, partial, x_own = call(
        soft_kernel, "soft",
        (shape((slots, tokens), F32), shape((3 * n_seq, own, width), BF16), shape((own, width), BF16)),
        (VMEM, HBM, VMEM),
        tuple(map(in_hbm, (combine_logits[0].T, grads, expert_out[0], router, slot_in[0]))), (HBM,) * 5,
        scratch=(pltpu.VMEM((slots, tokens), F32), held_tokens, pltpu.VMEM((2, own, width), BF16),
                 pltpu.VMEM((n_seq, own, width), BF16), SEMS((5,)), SEMS((n_seq,)), SEMS((n_seq,))),
    )
    every = lax.all_to_all(partial, "seq", split_axis=0, concat_axis=0, tiled=True)
    inputs = [x_own] + [shifted(x_own, n_grp, k) for k in range(1, n_grp)]
    gate, up = call(
        functools.partial(forward_kernel, n_grp), "forward", (shape(vec, F32), shape(vec, F32)), (VMEM, VMEM),
        (*inputs, in_hbm(w_gate), in_hbm(w_up)), (VMEM,) * n_grp + (HBM, HBM), scratch=(buf, buf, SEMS((2, own))),
        us=6, vmem=24 << 20,
    )
    slot_out = call(sum_kernel, "sum", shape((own, width), BF16), VMEM, (every, gate), (VMEM, VMEM), us=20)
    same = call(pause_kernel, "pause", shape((own, width), BF16), VMEM, (slot_out,), (VMEM,), us=20)
    all_out = [same] + [shifted(slot_out, n_grp, k) for k in range(1, n_grp)]
    *partials, up_grad, grad_down, grad_gate = call(
        functools.partial(middle_kernel, n_grp), "middle",
        (shape((own, width), F32),) + (shape((own, width), BF16),) * (n_grp - 1) + (shape(vec, BF16), big, big),
        (VMEM,) * (n_grp + 1) + (HBM, HBM),
        (*all_out, *inputs, gate, up, in_hbm(w_gate), w_up, w_down),
        (VMEM,) * (2 * n_grp + 2) + (HBM, VMEM, VMEM),
        scratch=(few, few, pltpu.VMEM((own, n_grp, width), F32), buf, buf, buf,
                 SEMS((own,)), sems, sems),
        us=8, vmem=32 << 20,
    )
    with jax.named_scope("back"):
        back = [shifted(partials[k], n_grp, n_grp - k) for k in range(1, n_grp)]
    with jax.named_scope("ending"):
        grad_up, token_grad, slot_grad = call(
            functools.partial(last_kernel, n_grp), "last",
            (big, shape((tokens, width), BF16), shape((own, width), F32)), (HBM, HBM, VMEM),
            (*inputs, up_grad, probs, in_hbm(grads), every, partials[0]),
            (VMEM,) * (n_grp + 2) + (HBM, VMEM, VMEM),
            scratch=(few, buf, held_tokens, held_tokens, sems, SEMS((2,))), us=5, vmem=24 << 20,
        )
    for part in back:
        slot_grad = slot_grad + part.astype(F32)
    return token_grad[None], slot_grad[None], grad_gate, grad_up, grad_down


def solution(mesh):
    def body(*args):
        return per_device(mesh.shape["seq"], mesh.shape["grp"], *args)

    tokens, weights = P("grp", "seq", None), P("seq", "grp", None)
    return jax.shard_map(
        body,
        mesh=mesh,
        in_specs=(tokens, tokens, tokens, tokens, P("seq", None), weights, weights, weights),
        out_specs=(tokens, tokens, weights, weights, weights),
        check_vma=False,
    )
```

```python
import functools

import jax
import jax.numpy as jnp
from jax import lax
from jax.experimental import pallas as pl
from jax.experimental.pallas import tpu as pltpu
from jax.sharding import PartitionSpec as P

F32 = jnp.float32
BF16 = jnp.bfloat16
VMEM = pl.BlockSpec(memory_space=pltpu.VMEM)
HBM = pl.BlockSpec(memory_space=pltpu.HBM)
SEMS = pltpu.SemaphoreType.DMA


def shape(dims, kind):
    return jax.ShapeDtypeStruct(dims, kind)


def in_hbm(x):
    return pltpu.with_memory_space_constraint(x, pltpu.HBM)


def dot(a, b, contract):
    return lax.dot_general(a, b, (contract, ((), ())), preferred_element_type=F32)


def start(src, dst, sem):
    copy = pltpu.make_async_copy(src, dst, sem)
    copy.start()
    return copy


def call(body, name, outs, out_specs, args, in_specs, scratch=(), us=1.0, vmem=8 << 20):
    return pl.pallas_call(
        body,
        name=name,
        out_shape=outs,
        in_specs=in_specs,
        out_specs=out_specs,
        scratch_shapes=scratch,
        compiler_params=pltpu.CompilerParams(vmem_limit_bytes=vmem),
        cost_estimate=pl.CostEstimate(flops=int(us * 8e8), bytes_accessed=int(us * 3e6), transcendentals=0),
    )(*args)


def soft_kernel(logits_hbm, grads_hbm, outputs_hbm, router_hbm, x_hbm, probs_ref, all_hbm, x_ref,
                logits_ref, grads_ref, both_ref, parts_ref, sems, both_sems, parts_sems):
    loads = [
        start(outputs_hbm, both_ref.at[0], sems.at[2]),
        start(router_hbm, both_ref.at[1], sems.at[3]),
        start(logits_hbm, logits_ref, sems.at[0]),
        start(grads_hbm, grads_ref, sems.at[1]),
        start(x_hbm, x_ref, sems.at[4]),
    ]
    n, own, _ = parts_ref.shape
    loads[0].wait()
    loads[1].wait()
    copies = [start(both_ref, all_hbm.at[pl.ds(3 * j + 1, 2)], both_sems.at[j]) for j in range(n)]
    loads[2].wait()
    logits = logits_ref[...]
    weights = jnp.exp(logits - jnp.max(logits, axis=0, keepdims=True))
    probs = weights / jnp.sum(weights, axis=0, keepdims=True)
    probs_ref[...] = probs
    loads[3].wait()
    partial = dot(probs.astype(BF16), grads_ref[...], ((1,), (0,))).astype(BF16)
    for j in range(n):
        parts_ref[j] = partial[j * own : (j + 1) * own]
    copies += [start(parts_ref.at[j], all_hbm.at[3 * j], parts_sems.at[j]) for j in range(n)]
    for copy in copies + loads[4:]:
        copy.wait()


def forward_kernel(n_grp, *refs):
    x_refs = refs[:n_grp]
    w_gate_hbm, w_up_hbm, gate_ref, up_ref, first_ref, w_gate_ref, w_up_ref, sems = refs[n_grp:]
    experts = gate_ref.shape[0]
    gates = [first_ref.at[0]] + [w_gate_ref.at[e] for e in range(experts - 1)]
    copies = []
    for e in range(experts):
        one = start(w_gate_hbm.at[e], gates[e], sems.at[0, e])
        copies.append((one, start(w_up_hbm.at[e], w_up_ref.at[e], sems.at[1, e])))
    for e in range(experts):
        x = jnp.concatenate([r[e : e + 1] for r in x_refs], axis=0)
        copies[e][0].wait()
        gate_ref[e] = dot(x, gates[e][...], ((1,), (1,)))
        copies[e][1].wait()
        up_ref[e] = dot(x, w_up_ref[e], ((1,), (1,)))


def sum_kernel(every_ref, after_ref, out_ref):
    del after_ref
    total = every_ref[0].astype(F32)
    for j in range(3, every_ref.shape[0], 3):
        total = total + every_ref[j].astype(F32)
    out_ref[...] = total.astype(BF16)


def pause_kernel(x_ref, same_ref):
    same_ref[...] = x_ref[...]


def outer_into(left, right, buf_ref, e, block=256):
    n, rows = left.shape
    pad = -n % 8
    tall = left if pad == 0 else jnp.concatenate([left, jnp.zeros((pad, rows), F32)], axis=0)
    tall, right = tall.T.astype(BF16), right.astype(BF16)
    block = min(block, rows)
    for b in range(0, rows, block):
        part = tall[b : b + block]
        total = part[:, 0:1] * right[0:1]
        for s in range(1, n):
            total = total + part[:, s : s + 1] * right[s : s + 1]
        buf_ref[e, pl.ds(b, block)] = total


def send(buf_ref, out_hbm, sems, e):
    blocks = sems.shape[1]
    block = buf_ref.shape[1] // blocks
    for b in range(blocks):
        span = pl.ds(b * block, block)
        start(buf_ref.at[e, span], out_hbm.at[e, span], sems.at[e, b])


def drain(out_hbm, buf_ref, sems):
    experts, blocks = sems.shape
    block = buf_ref.shape[1] // blocks

    @pl.loop(0, experts)
    def _(e):
        for b in range(blocks):
            span = pl.ds(b * block, block)
            pltpu.make_async_copy(buf_ref.at[e, span], out_hbm.at[e, span], sems.at[e, b]).wait()


def stack_rows(refs, into_ref):
    for e in range(into_ref.shape[0]):
        into_ref[e] = jnp.concatenate([r[e : e + 1] for r in refs], axis=0)


def middle_kernel(n_grp, *refs):
    so_refs, x_refs = refs[:n_grp], refs[n_grp : 2 * n_grp]
    gate_ref, up_ref, w_gate_hbm, w_up_ref, w_down_ref, first_ref = refs[2 * n_grp : 2 * n_grp + 6]
    partial_refs = refs[2 * n_grp + 6 : 3 * n_grp + 6]
    (up_grad_ref, grad_down_hbm, grad_gate_hbm, so_ref, x_ref, sum_ref, w_gate_ref, down_buf, gate_buf,
     w_gate_sems, down_sems, gate_sems) = refs[3 * n_grp + 6 :]
    experts = gate_ref.shape[0]

    def w_gate_copy(e):
        return pltpu.make_async_copy(w_gate_hbm.at[e], w_gate_ref.at[e - 1], w_gate_sems.at[e - 1])

    for e in range(1, experts):
        w_gate_copy(e).start()
    stack_rows(so_refs, so_ref)
    stack_rows(x_refs, x_ref)

    def hidden_grad_of(e):
        return dot(so_ref[e], w_down_ref[e], ((1,), (1,)))

    def step(e, hidden_grad):
        if e > 0:
            w_gate_copy(e).wait()
        w_gate = first_ref[0] if e == 0 else w_gate_ref[e - 1]
        gate, up = gate_ref[e], up_ref[e]
        sig = 1.0 / (1.0 + jnp.exp(-gate))
        hidden = (gate * sig * up).astype(BF16)
        up_grad = (hidden_grad * gate * sig).astype(BF16)
        gate_grad = (hidden_grad * up * sig * (1.0 + gate * (1.0 - sig))).astype(BF16)
        up_grad_ref[e] = up_grad
        later = hidden_grad_of(min(e + 1, experts - 1))
        sum_ref[e] = dot(gate_grad, w_gate, ((1,), (0,))) + dot(up_grad, w_up_ref[e], ((1,), (0,)))
        outer_into(hidden.astype(F32), so_ref[e].astype(F32), down_buf, e)
        outer_into(gate_grad.astype(F32), x_ref[e].astype(F32), gate_buf, e)
        send(down_buf, grad_down_hbm, down_sems, e)
        send(gate_buf, grad_gate_hbm, gate_sems, e)
        return later

    later = hidden_grad_of(0)
    for e in range(experts):
        later = step(e, later)
    for e in range(experts):
        for s, ref in enumerate(partial_refs):
            ref[e : e + 1] = sum_ref[e, s : s + 1].astype(ref.dtype)
    drain(grad_down_hbm, down_buf, down_sems)
    drain(grad_gate_hbm, gate_buf, gate_sems)


def last_kernel(n_grp, *refs):
    x_refs = refs[:n_grp]
    (up_grad_ref, probs_ref, grads_hbm, every_ref, partial_ref, grad_up_hbm, token_hbm, same_ref,
     x_ref, up_buf, grads_ref, token_ref, up_sems, sems) = refs[n_grp:]
    experts = up_grad_ref.shape[0]
    loaded = start(grads_hbm, grads_ref, sems.at[0])
    same_ref[...] = partial_ref[...]
    stack_rows(x_refs, x_ref)

    @pl.loop(0, experts)
    def _(e):
        outer_into(up_grad_ref[e].astype(F32), x_ref[e].astype(F32), up_buf, e)
        send(up_buf, grad_up_hbm, up_sems, e)

    probs = probs_ref[...]
    n = every_ref.shape[0] // 3
    outputs = jnp.concatenate([every_ref[3 * j + 1] for j in range(n)], axis=0)
    routers = jnp.concatenate([every_ref[3 * j + 2] for j in range(n)], axis=0)
    loaded.wait()
    weight_grad = dot(outputs, grads_ref[...], ((1,), (1,)))
    centre = jnp.sum(weight_grad * probs, axis=0, keepdims=True)
    logit_grad = (probs * (weight_grad - centre)).astype(BF16)
    token_ref[...] = dot(logit_grad, routers, ((0,), (0,))).astype(BF16)
    tokens = start(token_ref, token_hbm, sems.at[1])
    drain(grad_up_hbm, up_buf, up_sems)
    tokens.wait()


def shifted(x, size, k):
    return lax.ppermute(x, "grp", [((i + k) % size, i) for i in range(size)])


def per_device(n_seq, n_grp, out_grad, combine_logits, expert_out, slot_in, router, w_gate, w_up, w_down):
    grads = out_grad[0]
    own, width = router.shape
    rows = w_gate.shape[1]
    tokens = grads.shape[0]
    slots = n_seq * own
    block = min(256, rows)
    vec = (own, n_grp, rows)
    held = pltpu.VMEM((own, rows, width), BF16)
    big = shape((own, rows, width), BF16)
    buf = pltpu.VMEM((own, rows, width), BF16)
    few = pltpu.VMEM((own, n_grp, width), BF16)
    held_tokens = pltpu.VMEM((tokens, width), BF16)
    sems = SEMS((own, rows // block))
    probs, partial, x_own = call(
        soft_kernel, "soft",
        (shape((slots, tokens), F32), shape((3 * n_seq, own, width), BF16), shape((own, width), BF16)),
        (VMEM, HBM, VMEM),
        tuple(map(in_hbm, (combine_logits[0].T, grads, expert_out[0], router, slot_in[0]))), (HBM,) * 5,
        scratch=(pltpu.VMEM((slots, tokens), F32), held_tokens, pltpu.VMEM((2, own, width), BF16),
                 pltpu.VMEM((n_seq, own, width), BF16), SEMS((5,)), SEMS((n_seq,)), SEMS((n_seq,))),
    )
    every = lax.all_to_all(partial, "seq", split_axis=0, concat_axis=0, tiled=True)
    inputs = [x_own] + [shifted(x_own, n_grp, k) for k in range(1, n_grp)]
    gate, up, w_first = call(
        functools.partial(forward_kernel, n_grp), "forward",
        (shape(vec, F32), shape(vec, F32), pltpu.VMEM((1, rows, width), BF16)), (VMEM,) * 3,
        (*inputs, in_hbm(w_gate), in_hbm(w_up)), (VMEM,) * n_grp + (HBM, HBM),
        scratch=(pltpu.VMEM((own - 1, rows, width), BF16), buf, SEMS((2, own))),
        us=6, vmem=24 << 20,
    )
    slot_out = call(sum_kernel, "sum", shape((own, width), BF16), VMEM, (every, gate), (VMEM, VMEM), us=20)
    same = call(pause_kernel, "pause", shape((own, width), BF16), VMEM, (slot_out,), (VMEM,), us=20)
    all_out = [same] + [shifted(slot_out, n_grp, k) for k in range(1, n_grp)]
    *partials, up_grad, grad_down, grad_gate = call(
        functools.partial(middle_kernel, n_grp), "middle",
        (shape((own, width), F32),) + (shape((own, width), BF16),) * (n_grp - 1) + (shape(vec, BF16), big, big),
        (VMEM,) * (n_grp + 1) + (HBM, HBM),
        (*all_out, *inputs, gate, up, in_hbm(w_gate), w_up, w_down, w_first),
        (VMEM,) * (2 * n_grp + 2) + (HBM, VMEM, VMEM, VMEM),
        scratch=(few, few, pltpu.VMEM((own, n_grp, width), F32), pltpu.VMEM((own - 1, rows, width), BF16),
                 buf, buf, SEMS((own - 1,)), sems, sems),
        us=8, vmem=32 << 20,
    )
    with jax.named_scope("back"):
        back = [shifted(partials[k], n_grp, n_grp - k) for k in range(1, n_grp)]
    with jax.named_scope("ending"):
        grad_up, token_grad, slot_grad = call(
            functools.partial(last_kernel, n_grp), "last",
            (big, shape((tokens, width), BF16), shape((own, width), F32)), (HBM, HBM, VMEM),
            (*inputs, up_grad, probs, in_hbm(grads), every, partials[0]),
            (VMEM,) * (n_grp + 2) + (HBM, VMEM, VMEM),
            scratch=(few, buf, held_tokens, held_tokens, sems, SEMS((2,))), us=5, vmem=24 << 20,
        )
    for part in back:
        slot_grad = slot_grad + part.astype(F32)
    return token_grad[None], slot_grad[None], grad_gate, grad_up, grad_down


def solution(mesh):
    def body(*args):
        return per_device(mesh.shape["seq"], mesh.shape["grp"], *args)

    tokens, weights = P("grp", "seq", None), P("seq", "grp", None)
    return jax.shard_map(
        body,
        mesh=mesh,
        in_specs=(tokens, tokens, tokens, tokens, P("seq", None), weights, weights, weights),
        out_specs=(tokens, tokens, weights, weights, weights),
        check_vma=False,
    )
```

```python
import functools

import jax
import jax.numpy as jnp
from jax import lax
from jax.experimental import pallas as pl
from jax.experimental.pallas import tpu as pltpu
from jax.sharding import PartitionSpec as P

F32 = jnp.float32
BF16 = jnp.bfloat16
VMEM = pl.BlockSpec(memory_space=pltpu.VMEM)
HBM = pl.BlockSpec(memory_space=pltpu.HBM)
SEMS = pltpu.SemaphoreType.DMA


def shape(dims, kind):
    return jax.ShapeDtypeStruct(dims, kind)


def in_hbm(x):
    return pltpu.with_memory_space_constraint(x, pltpu.HBM)


def dot(a, b, contract):
    return lax.dot_general(a, b, (contract, ((), ())), preferred_element_type=F32)


def start(src, dst, sem):
    copy = pltpu.make_async_copy(src, dst, sem)
    copy.start()
    return copy


def call(body, name, outs, out_specs, args, in_specs, scratch=(), us=1.0, vmem=8 << 20):
    return pl.pallas_call(
        body,
        name=name,
        out_shape=outs,
        in_specs=in_specs,
        out_specs=out_specs,
        scratch_shapes=scratch,
        compiler_params=pltpu.CompilerParams(vmem_limit_bytes=vmem),
        cost_estimate=pl.CostEstimate(flops=int(us * 8e8), bytes_accessed=int(us * 3e6), transcendentals=0),
    )(*args)


def soft_kernel(logits_hbm, grads_hbm, outputs_hbm, router_hbm, x_hbm, probs_ref, all_hbm, x_ref, grads_ref,
                logits_ref, both_ref, parts_ref, sems, both_sems, parts_sems):
    loads = [
        start(outputs_hbm, both_ref.at[0], sems.at[2]),
        start(router_hbm, both_ref.at[1], sems.at[3]),
        start(logits_hbm, logits_ref, sems.at[0]),
        start(grads_hbm, grads_ref, sems.at[1]),
        start(x_hbm, x_ref, sems.at[4]),
    ]
    n, own, _ = parts_ref.shape
    loads[0].wait()
    loads[1].wait()
    copies = [start(both_ref, all_hbm.at[pl.ds(3 * j + 1, 2)], both_sems.at[j]) for j in range(n)]
    loads[2].wait()
    logits = logits_ref[...]
    weights = jnp.exp(logits - jnp.max(logits, axis=0, keepdims=True))
    probs = weights / jnp.sum(weights, axis=0, keepdims=True)
    probs_ref[...] = probs
    loads[3].wait()
    partial = dot(probs.astype(BF16), grads_ref[...], ((1,), (0,))).astype(BF16)
    for j in range(n):
        parts_ref[j] = partial[j * own : (j + 1) * own]
    copies += [start(parts_ref.at[j], all_hbm.at[3 * j], parts_sems.at[j]) for j in range(n)]
    for copy in copies + loads[4:]:
        copy.wait()


def forward_kernel(n_grp, *refs):
    x_refs = refs[:n_grp]
    w_gate_hbm, w_up_hbm, gate_ref, up_ref, first_ref, w_gate_ref, w_up_ref, sems = refs[n_grp:]
    experts = gate_ref.shape[0]
    gates = [first_ref.at[0]] + [w_gate_ref.at[e] for e in range(experts - 1)]
    copies = []
    for e in range(experts):
        one = start(w_gate_hbm.at[e], gates[e], sems.at[0, e])
        copies.append((one, start(w_up_hbm.at[e], w_up_ref.at[e], sems.at[1, e])))
    for e in range(experts):
        x = jnp.concatenate([r[e : e + 1] for r in x_refs], axis=0)
        copies[e][0].wait()
        gate_ref[e] = dot(x, gates[e][...], ((1,), (1,)))
        copies[e][1].wait()
        up_ref[e] = dot(x, w_up_ref[e], ((1,), (1,)))


def sum_kernel(every_ref, after_ref, out_ref):
    del after_ref
    total = every_ref[0].astype(F32)
    for j in range(3, every_ref.shape[0], 3):
        total = total + every_ref[j].astype(F32)
    out_ref[...] = total.astype(BF16)


def pause_kernel(x_ref, same_ref):
    same_ref[...] = x_ref[...]


def outer_into(left, right, buf_ref, e, block=256):
    n, rows = left.shape
    pad = -n % 8
    tall = left if pad == 0 else jnp.concatenate([left, jnp.zeros((pad, rows), F32)], axis=0)
    tall, right = tall.T.astype(BF16), right.astype(BF16)
    block = min(block, rows)
    for b in range(0, rows, block):
        part = tall[b : b + block]
        total = part[:, 0:1] * right[0:1]
        for s in range(1, n):
            total = total + part[:, s : s + 1] * right[s : s + 1]
        buf_ref[e, pl.ds(b, block)] = total


def send(buf_ref, out_hbm, sems, e):
    blocks = sems.shape[1]
    block = buf_ref.shape[1] // blocks
    for b in range(blocks):
        span = pl.ds(b * block, block)
        start(buf_ref.at[e, span], out_hbm.at[e, span], sems.at[e, b])


def drain(out_hbm, buf_ref, sems):
    experts, blocks = sems.shape
    block = buf_ref.shape[1] // blocks

    @pl.loop(0, experts)
    def _(e):
        for b in range(blocks):
            span = pl.ds(b * block, block)
            pltpu.make_async_copy(buf_ref.at[e, span], out_hbm.at[e, span], sems.at[e, b]).wait()


def stack_rows(refs, into_ref):
    for e in range(into_ref.shape[0]):
        into_ref[e] = jnp.concatenate([r[e : e + 1] for r in refs], axis=0)


def middle_kernel(n_grp, *refs):
    so_refs, x_refs = refs[:n_grp], refs[n_grp : 2 * n_grp]
    gate_ref, up_ref, w_gate_hbm, w_up_ref, w_down_ref, first_ref = refs[2 * n_grp : 2 * n_grp + 6]
    partial_refs = refs[2 * n_grp + 6 : 3 * n_grp + 6]
    (up_grad_ref, grad_down_hbm, grad_gate_hbm, so_ref, x_ref, sum_ref, w_gate_ref, down_buf, gate_buf,
     w_gate_sems, down_sems, gate_sems) = refs[3 * n_grp + 6 :]
    experts = gate_ref.shape[0]

    def w_gate_copy(e):
        return pltpu.make_async_copy(w_gate_hbm.at[e], w_gate_ref.at[e - 1], w_gate_sems.at[e - 1])

    for e in range(1, experts):
        w_gate_copy(e).start()
    stack_rows(so_refs, so_ref)
    stack_rows(x_refs, x_ref)

    def hidden_grad_of(e):
        return dot(so_ref[e], w_down_ref[e], ((1,), (1,)))

    def step(e, hidden_grad):
        if e > 0:
            w_gate_copy(e).wait()
        w_gate = first_ref[0] if e == 0 else w_gate_ref[e - 1]
        gate, up = gate_ref[e], up_ref[e]
        sig = 1.0 / (1.0 + jnp.exp(-gate))
        hidden = (gate * sig * up).astype(BF16)
        up_grad = (hidden_grad * gate * sig).astype(BF16)
        gate_grad = (hidden_grad * up * sig * (1.0 + gate * (1.0 - sig))).astype(BF16)
        up_grad_ref[e] = up_grad
        later = hidden_grad_of(min(e + 1, experts - 1))
        sum_ref[e] = dot(gate_grad, w_gate, ((1,), (0,))) + dot(up_grad, w_up_ref[e], ((1,), (0,)))
        outer_into(hidden.astype(F32), so_ref[e].astype(F32), down_buf, e)
        outer_into(gate_grad.astype(F32), x_ref[e].astype(F32), gate_buf, e)
        send(down_buf, grad_down_hbm, down_sems, e)
        send(gate_buf, grad_gate_hbm, gate_sems, e)
        return later

    later = hidden_grad_of(0)
    for e in range(experts):
        later = step(e, later)
    for e in range(experts):
        for s, ref in enumerate(partial_refs):
            ref[e : e + 1] = sum_ref[e, s : s + 1].astype(ref.dtype)
    drain(grad_down_hbm, down_buf, down_sems)
    drain(grad_gate_hbm, gate_buf, gate_sems)


def last_kernel(n_grp, *refs):
    x_refs = refs[:n_grp]
    (up_grad_ref, probs_ref, grads_ref, every_ref, partial_ref, grad_up_hbm, token_hbm, same_ref,
     x_ref, up_buf, token_ref, up_sems, sems) = refs[n_grp:]
    experts = up_grad_ref.shape[0]
    same_ref[...] = partial_ref[...]
    stack_rows(x_refs, x_ref)

    @pl.loop(0, experts)
    def _(e):
        outer_into(up_grad_ref[e].astype(F32), x_ref[e].astype(F32), up_buf, e)
        send(up_buf, grad_up_hbm, up_sems, e)

    probs = probs_ref[...]
    n = every_ref.shape[0] // 3
    outputs = jnp.concatenate([every_ref[3 * j + 1] for j in range(n)], axis=0)
    routers = jnp.concatenate([every_ref[3 * j + 2] for j in range(n)], axis=0)
    weight_grad = dot(outputs, grads_ref[...], ((1,), (1,)))
    centre = jnp.sum(weight_grad * probs, axis=0, keepdims=True)
    logit_grad = (probs * (weight_grad - centre)).astype(BF16)
    token_ref[...] = dot(logit_grad, routers, ((0,), (0,))).astype(BF16)
    tokens = start(token_ref, token_hbm, sems.at[1])
    drain(grad_up_hbm, up_buf, up_sems)
    tokens.wait()


def shifted(x, size, k):
    return lax.ppermute(x, "grp", [((i + k) % size, i) for i in range(size)])


def per_device(n_seq, n_grp, out_grad, combine_logits, expert_out, slot_in, router, w_gate, w_up, w_down):
    grads = out_grad[0]
    own, width = router.shape
    rows = w_gate.shape[1]
    tokens = grads.shape[0]
    slots = n_seq * own
    block = min(512, rows)
    vec = (own, n_grp, rows)
    held = pltpu.VMEM((own, rows, width), BF16)
    big = shape((own, rows, width), BF16)
    buf = pltpu.VMEM((own, rows, width), BF16)
    few = pltpu.VMEM((own, n_grp, width), BF16)
    held_tokens = pltpu.VMEM((tokens, width), BF16)
    sems = SEMS((own, rows // block))
    probs, partial, x_own, grads_v = call(
        soft_kernel, "soft",
        (shape((slots, tokens), F32), shape((3 * n_seq, own, width), BF16), shape((own, width), BF16),
         pltpu.VMEM((tokens, width), BF16)),
        (VMEM, HBM, VMEM, VMEM),
        tuple(map(in_hbm, (combine_logits[0].T, grads, expert_out[0], router, slot_in[0]))), (HBM,) * 5,
        scratch=(pltpu.VMEM((slots, tokens), F32), pltpu.VMEM((2, own, width), BF16),
                 pltpu.VMEM((n_seq, own, width), BF16), SEMS((5,)), SEMS((n_seq,)), SEMS((n_seq,))),
    )
    every = lax.all_to_all(partial, "seq", split_axis=0, concat_axis=0, tiled=True)
    inputs = [x_own] + [shifted(x_own, n_grp, k) for k in range(1, n_grp)]
    gate, up, w_first = call(
        functools.partial(forward_kernel, n_grp), "forward",
        (shape(vec, F32), shape(vec, F32), pltpu.VMEM((1, rows, width), BF16)), (VMEM,) * 3,
        (*inputs, in_hbm(w_gate), in_hbm(w_up)), (VMEM,) * n_grp + (HBM, HBM),
        scratch=(pltpu.VMEM((own - 1, rows, width), BF16), buf, SEMS((2, own))),
        us=6, vmem=24 << 20,
    )
    slot_out = call(sum_kernel, "sum", shape((own, width), BF16), VMEM, (every, gate), (VMEM, VMEM), us=20)
    same = call(pause_kernel, "pause", shape((own, width), BF16), VMEM, (slot_out,), (VMEM,), us=20)
    all_out = [same] + [shifted(slot_out, n_grp, k) for k in range(1, n_grp)]
    *partials, up_grad, grad_down, grad_gate = call(
        functools.partial(middle_kernel, n_grp), "middle",
        (shape((own, width), F32),) + (shape((own, width), BF16),) * (n_grp - 1) + (shape(vec, BF16), big, big),
        (VMEM,) * (n_grp + 1) + (HBM, HBM),
        (*all_out, *inputs, gate, up, in_hbm(w_gate), w_up, w_down, w_first),
        (VMEM,) * (2 * n_grp + 2) + (HBM, VMEM, VMEM, VMEM),
        scratch=(few, few, pltpu.VMEM((own, n_grp, width), F32), pltpu.VMEM((own - 1, rows, width), BF16),
                 buf, buf, SEMS((own - 1,)), sems, sems),
        us=8, vmem=32 << 20,
    )
    with jax.named_scope("back"):
        back = [shifted(partials[k], n_grp, n_grp - k) for k in range(1, n_grp)]
    with jax.named_scope("ending"):
        grad_up, token_grad, slot_grad = call(
            functools.partial(last_kernel, n_grp), "last",
            (big, shape((tokens, width), BF16), shape((own, width), F32)), (HBM, HBM, VMEM),
            (*inputs, up_grad, probs, grads_v, every, partials[0]),
            (VMEM,) * (n_grp + 5),
            scratch=(few, buf, held_tokens, sems, SEMS((2,))), us=5, vmem=24 << 20,
        )
    for part in back:
        slot_grad = slot_grad + part.astype(F32)
    return token_grad[None], slot_grad[None], grad_gate, grad_up, grad_down


def solution(mesh):
    def body(*args):
        return per_device(mesh.shape["seq"], mesh.shape["grp"], *args)

    tokens, weights = P("grp", "seq", None), P("seq", "grp", None)
    return jax.shard_map(
        body,
        mesh=mesh,
        in_specs=(tokens, tokens, tokens, tokens, P("seq", None), weights, weights, weights),
        out_specs=(tokens, tokens, weights, weights, weights),
        check_vma=False,
    )
```
